256 devices in a mesh: seq: 16 (over y, x), width: 16 (over z, core).
Axes of the slice: x: 4, y: 4, z: 8, core: 2. Of those that a mesh axis runs over, the one named last changes fastest.
Arguments:
- leak_rate: float32 [1, 32768, 2048], P(None, 'seq', 'width'), may hold values from 0.2 to 2
- signal_in: bfloat16 [1, 32768, 2048], P(None, 'seq', 'width'), may hold values from -6 to 6
- norm_gain: float32 [2048], P('width'), may hold values from 0.25 to 1.75
Outputs:
- mixed_out: bfloat16 [1, 32768, 2048], P(None, 'seq', 'width')
The draws below stay inside these ranges and needn't reach their ends.
All inputs are finite; a program needn't handle non-finite values.
Results may differ from the reference program's by a relative error of at most 0.001.
Values sent between devices are 32-bit elements; how exact they have to be, the bound alone decides.
A program may use at most 64 MiB of HBM per device.

```python
import jax
import jax.numpy as jnp
from jax import lax

BATCH = 1
CHANNELS = 2048
LENGTH = 32768


def steps_of(own_key, dims, cuts, low, high):
    def one(position, blocks):
        heights = jax.random.uniform(jax.random.fold_in(jax.random.fold_in(own_key, 6), position), (blocks,), jnp.float32, low / len(cuts), high / len(cuts))
        return jnp.repeat(jnp.exp(heights), dims[position] // blocks).reshape((-1,) + (1,) * (len(dims) - position - 1))

    factor_of = one(*cuts[0])
    for cut in cuts[1:]:
        factor_of = factor_of * one(*cut)
    return factor_of


def bell_draw(rng, shape, scale, limit, shards=(), held_as=jnp.bfloat16):
    loudness = steps_of(rng, shape, shards, -0.22, 0.18) if shards else 1.0
    drawn = jax.random.normal(rng, shape, jnp.float32) * scale * loudness
    return jnp.minimum(jnp.maximum(drawn, -limit), limit).astype(held_as)


def setup_inputs(seed: int = 0) -> dict:
    seeds = jax.random.split(jax.random.key(seed), 4)
    leak_rate = jnp.clip(0.2 + 1.8 * jax.random.uniform(seeds[0], (BATCH, LENGTH, CHANNELS), jnp.float32) ** steps_of(seeds[0], (BATCH, LENGTH, CHANNELS), ((1, 16), (2, 16)), -0.2, 0.2), 0.2, 2.0)
    signal_in = bell_draw(seeds[1], (BATCH, LENGTH, CHANNELS), 1.0, 6.0, ((1, 16), (2, 16)))
    norm_gain = jnp.clip(1.0 + 0.15 * jax.random.normal(seeds[2], (CHANNELS,), jnp.float32), 0.25, 1.75)
    return {"leak_rate": leak_rate, "signal_in": signal_in, "norm_gain": norm_gain}


def join_pair(earlier, later):
    return (earlier[0] * later[0], later[0] * earlier[1] + later[1])

def reference(leak_rate, signal_in, norm_gain):
    keep = jnp.exp(-leak_rate / LENGTH)
    push = signal_in.astype(jnp.float32) * LENGTH ** (-0.5)
    forward = lax.associative_scan(join_pair, (keep, push), axis=1)[1]
    backward = lax.associative_scan(join_pair, (keep, push), axis=1, reverse=True)[1]
    states = forward + backward
    power = lax.optimization_barrier(jnp.mean(states * states, axis=-1, keepdims=True))
    mixed_out = (states * lax.rsqrt(power + 1e-06) * norm_gain).astype(jnp.bfloat16)
    return mixed_out
```

```python
import functools

import jax
import jax.numpy as jnp
from jax import lax
from jax.experimental import pallas as pl
from jax.experimental.pallas import tpu as pltpu
from jax.sharding import PartitionSpec as P

MESH = pl.DeviceIdType.MESH
ROWS = 128
NT = (((1,), (1,)), ((), ()))


def ring_order(sizes):
    offsets = [()]
    for n in sizes:
        offsets = [o + (d,) for o in offsets for d in range(n)]
    far = lambda o: sum(min(d, n - d) for d, n in zip(o, sizes))
    return sorted((o for o in offsets if any(o)), key=lambda o: -far(o))


def split(x):
    high = x.astype(jnp.bfloat16)
    return high, (x - high.astype(jnp.float32)).astype(jnp.bfloat16)


def kernel(
    length, channels, seq_sizes, width_sizes,
    leak_hbm, signal_hbm, gain_ref, out_hbm,
    leak, signal, decay, grow, states, out,
    carried_f, decayed_f, carried_b, decayed_b,
    own_carry, got_carry, own_power, got_power,
    in_sem, out_sem, carry_send, carry_recv, power_send, power_recv,
):
    f32 = jnp.float32
    seq_n, width_n = seq_sizes[0] * seq_sizes[1], width_sizes[0] * width_sizes[1]
    seq, width = lax.axis_index("seq"), lax.axis_index("width")
    blocks = leak.shape[0] // ROWS

    def partner(here, sizes, offset):
        major = lax.rem(here // sizes[1] + offset[0], sizes[0])
        minor = lax.rem(lax.rem(here, sizes[1]) + offset[1], sizes[1])
        return major * sizes[1] + minor

    seq_partners = [partner(seq, seq_sizes, o) for o in ring_order(seq_sizes)]
    width_partners = [partner(width, width_sizes, o) for o in ring_order(width_sizes)]

    barrier = pltpu.get_barrier_semaphore()
    for other in seq_partners:
        pl.semaphore_signal(barrier, inc=1, device_id={"seq": other}, device_id_type=MESH)
    for other in width_partners:
        pl.semaphore_signal(barrier, inc=1, device_id={"width": other}, device_id_type=MESH)
    parts = in_sem.shape[1]
    part = leak.shape[0] // parts
    loads = []
    for k in range(parts):
        rows = pl.ds(k * part, part)
        loads.append((
            pltpu.make_async_copy(leak_hbm.at[rows], leak.at[rows], in_sem.at[0, k]),
            pltpu.make_async_copy(signal_hbm.at[rows], signal.at[rows], in_sem.at[1, k]),
        ))
        for load in loads[-1]:
            load.start()

    row = lax.broadcasted_iota(jnp.int32, (ROWS, ROWS), 0)
    col = lax.broadcasted_iota(jnp.int32, (ROWS, ROWS), 1)
    upto = jnp.where(col <= row, 1.0, 0.0).astype(jnp.bfloat16)
    upto = jnp.concatenate([upto, upto], axis=1)

    ends, sums_f, sums_b = [], [], []
    for pair in range(blocks // 2):
        if (pair * 2 * ROWS) % part == 0:
            for load in loads[pair * 2 * ROWS // part]:
                load.wait()
        two = [pl.ds((2 * pair + side) * ROWS, ROWS) for side in (0, 1)]
        steps = [leak[rows] * (1.0 / length) for rows in two]
        pieces = [split(step) for step in steps]
        summed = jnp.dot(
            upto,
            jnp.concatenate(
                [jnp.concatenate([p[k] for p in pieces], axis=1) for k in (0, 1)], axis=0
            ),
            preferred_element_type=f32,
        )
        for side in (0, 1):
            rows = two[side]
            through = summed[:, side * ROWS : (side + 1) * ROWS]
            before = through - steps[side]
            push = signal[rows]
            wide = push.astype(f32)
            extra_f = (wide * (jnp.exp(through) - 1.0)).astype(jnp.bfloat16)
            extra_b = (wide * (jnp.exp(-before) - 1.0)).astype(jnp.bfloat16)
            both = jnp.dot(
                upto,
                jnp.concatenate(
                    [
                        jnp.concatenate([push, push], axis=1),
                        jnp.concatenate([extra_f, extra_b], axis=1),
                    ],
                    axis=0,
                ),
                preferred_element_type=f32,
            )
            down, up = jnp.exp(-through), jnp.exp(before)
            sum_f, sum_b = both[:, :ROWS], both[:, ROWS:]
            decay[rows] = down
            grow[rows] = up
            states[rows] = down * sum_f + (wide - up * sum_b)
            ends.append(down[ROWS - 1 :])
            sums_f.append(down[ROWS - 1 :] * sum_f[ROWS - 1 :])
            sums_b.append(sum_b[ROWS - 1 :])

    at, product = jnp.zeros_like(ends[0]), jnp.ones_like(ends[0])
    for b in range(blocks):
        carried_f[b : b + 1] = at
        decayed_f[b : b + 1] = product
        at, product = at * ends[b] + sums_f[b], product * ends[b]
    own_carry[0:1] = product
    own_carry[1:2] = at
    at, product = jnp.zeros_like(ends[0]), jnp.ones_like(ends[0])
    for b in reversed(range(blocks)):
        at, product = at * ends[b] + sums_b[b], product * ends[b]
        carried_b[b : b + 1] = at
        decayed_b[b : b + 1] = product
    own_carry[2:3] = at
    got_carry[seq] = own_carry[...]

    pl.semaphore_wait(barrier, seq_n + width_n - 2)

    sends = []
    for k, other in enumerate(seq_partners):
        sends.append(pltpu.make_async_remote_copy(
            src_ref=own_carry, dst_ref=got_carry.at[seq],
            send_sem=carry_send.at[k], recv_sem=carry_recv.at[k],
            device_id={"seq": other}, device_id_type=MESH,
        ))
        sends[-1].start()
    for send in sends:
        send.wait_recv()

    into_f, into_b = jnp.zeros_like(ends[0]), jnp.zeros_like(ends[0])
    for j in range(seq_n):
        into_f = jnp.where(j < seq, into_f * got_carry[j, 0:1] + got_carry[j, 1:2], into_f)
        i = seq_n - 1 - j
        into_b = jnp.where(i > seq, into_b * got_carry[i, 0:1] + got_carry[i, 2:3], into_b)
    carried_f[...] = carried_f[...] + decayed_f[...] * into_f
    carried_b[...] = carried_b[...] + decayed_b[...] * into_b

    ones = jnp.ones((8, 2 * ROWS), jnp.bfloat16)
    for pair in range(blocks // 2):
        squares = []
        for b in (2 * pair, 2 * pair + 1):
            rows = pl.ds(b * ROWS, ROWS)
            value = (
                states[rows]
                + decay[rows] * carried_f[b : b + 1]
                + grow[rows] * carried_b[b : b + 1]
            )
            states[rows] = value
            squares.append(jnp.concatenate(split(value * value), axis=1))
        power = lax.dot_general(
            ones, jnp.concatenate(squares, axis=0), NT, preferred_element_type=f32
        )
        own_power[2 * pair : 2 * pair + 1] = power[0:1, :ROWS]
        own_power[2 * pair + 1 : 2 * pair + 2] = power[0:1, ROWS:]
    got_power[width] = own_power[...]

    for k, other in enumerate(width_partners):
        send = pltpu.make_async_remote_copy(
            src_ref=own_power, dst_ref=got_power.at[width],
            send_sem=power_send.at[k], recv_sem=power_recv.at[k],
            device_id={"width": other}, device_id_type=MESH,
        )
        send.start()
        sends.append(send)

    gain = gain_ref[...] * length**-0.5
    for b in range(blocks):
        rows = pl.ds(b * ROWS, ROWS)
        states[rows] = states[rows] * gain

    for send in sends[seq_n - 1 :]:
        send.wait_recv()
    total = got_power[0]
    for j in range(1, width_n):
        total = total + got_power[j]
    scale = lax.rsqrt(total * (1.0 / (channels * length)) + 1e-06)
    scale = jnp.concatenate([scale, jnp.zeros((ROWS - blocks, ROWS), f32)], axis=0).T

    parts = out_sem.shape[0]
    part = leak.shape[0] // parts
    stores = []
    for b in range(blocks):
        rows = pl.ds(b * ROWS, ROWS)
        out[rows] = (states[rows] * scale[:, b : b + 1]).astype(out.dtype)
        if (b + 1) * ROWS % part == 0:
            k = (b + 1) * ROWS // part - 1
            rows = pl.ds(k * part, part)
            stores.append(pltpu.make_async_copy(out.at[rows], out_hbm.at[rows], out_sem.at[k]))
            stores[-1].start()
    for send in sends:
        send.wait_send()
    for store in stores:
        store.wait()


def solution(mesh):
    sizes = dict(mesh.shape)
    seq_n, width_n = sizes["seq"], sizes["width"]
    seq_sizes, width_sizes = (4, seq_n // 4), (width_n // 2, 2)

    def per_device(leak_rate, signal_in, norm_gain):
        _, rows, lanes = leak_rate.shape
        length, channels = rows * seq_n, lanes * width_n
        blocks = rows // ROWS
        f32 = jnp.float32
        vmem, dma = pltpu.VMEM, pltpu.SemaphoreType.DMA
        out = pl.pallas_call(
            functools.partial(kernel, length, channels, seq_sizes, width_sizes),
            out_shape=jax.ShapeDtypeStruct((rows, lanes), jnp.bfloat16),
            in_specs=[
                pl.BlockSpec(memory_space=pl.ANY),
                pl.BlockSpec(memory_space=pl.ANY),
                pl.BlockSpec(memory_space=pltpu.VMEM),
            ],
            out_specs=pl.BlockSpec(memory_space=pl.ANY),
            scratch_shapes=[
                vmem((rows, lanes), f32),
                vmem((rows, lanes), jnp.bfloat16),
                vmem((rows, lanes), f32),
                vmem((rows, lanes), f32),
                vmem((rows, lanes), f32),
                vmem((rows, lanes), jnp.bfloat16),
                vmem((blocks, lanes), f32),
                vmem((blocks, lanes), f32),
                vmem((blocks, lanes), f32),
                vmem((blocks, lanes), f32),
                vmem((3, lanes), f32),
                vmem((seq_n, 3, lanes), f32),
                vmem((blocks, lanes), f32),
                vmem((width_n, blocks, lanes), f32),
                dma((2, 4)),
                dma((4,)),
                dma((seq_n - 1,)),
                dma((seq_n - 1,)),
                dma((width_n - 1,)),
                dma((width_n - 1,)),
            ],
            compiler_params=pltpu.CompilerParams(collective_id=0, has_side_effects=True),
            name="scan_norm",
        )(leak_rate[0], signal_in[0], norm_gain[None])
        return out[None]

    return jax.shard_map(
        per_device,
        mesh=mesh,
        in_specs=(P(None, "seq", "width"), P(None, "seq", "width"), P("width")),
        out_specs=P(None, "seq", "width"),
        check_vma=False,
    )
```

```python
import functools
import math

import jax
import jax.numpy as jnp
from jax import lax
from jax.experimental import pallas as pl
from jax.experimental.pallas import tpu as pltpu
from jax.sharding import PartitionSpec as P

MESH = pl.DeviceIdType.MESH
ROWS = 128
NT = (((1,), (1,)), ((), ()))


def ring_order(sizes):
    offsets = [()]
    for n in sizes:
        offsets = [o + (d,) for o in offsets for d in range(n)]
    far = lambda o: sum(min(d, n - d) for d, n in zip(o, sizes))
    return sorted((o for o in offsets if any(o)), key=lambda o: -far(o))


def split(x):
    high = x.astype(jnp.bfloat16)
    return high, (x - high.astype(jnp.float32)).astype(jnp.bfloat16)


def kernel(
    length, channels, seq_sizes, width_sizes,
    leak_hbm, signal_hbm, gain_hbm, states, scale_ref,
    leak, signal, gain, through, grow_f, grow_b, decay, grow,
    carried_f, decayed_f, carried_b, decayed_b,
    own_carry, got_carry, own_power, got_power,
    in_sem, gain_sem, carry_send, carry_recv, power_send, power_recv,
):
    f32 = jnp.float32
    seq_n, width_n = seq_sizes[0] * seq_sizes[1], width_sizes[0] * width_sizes[1]
    seq, width = lax.axis_index("seq"), lax.axis_index("width")
    blocks = leak.shape[0] // ROWS

    def partner(here, sizes, offset):
        major = lax.rem(here // sizes[1] + offset[0], sizes[0])
        minor = lax.rem(lax.rem(here, sizes[1]) + offset[1], sizes[1])
        return major * sizes[1] + minor

    seq_partners = [partner(seq, seq_sizes, o) for o in ring_order(seq_sizes)]
    width_partners = [partner(width, width_sizes, o) for o in ring_order(width_sizes)]

    with jax.named_scope("greet"):
        barrier = pltpu.get_barrier_semaphore()
        for other in seq_partners:
            pl.semaphore_signal(barrier, inc=1, device_id={"seq": other}, device_id_type=MESH)
        for other in width_partners:
            pl.semaphore_signal(barrier, inc=1, device_id={"width": other}, device_id_type=MESH)
        parts = in_sem.shape[1]
        part = leak.shape[0] // parts
        loads = []
        for k in range(parts):
            rows = pl.ds(k * part, part)
            loads.append((
                pltpu.make_async_copy(leak_hbm.at[rows], leak.at[rows], in_sem.at[0, k]),
                pltpu.make_async_copy(signal_hbm.at[rows], signal.at[rows], in_sem.at[1, k]),
            ))
            for load in loads[-1]:
                load.start()
        gain_load = pltpu.make_async_copy(gain_hbm, gain, gain_sem)
        gain_load.start()


    row = lax.broadcasted_iota(jnp.int32, (ROWS, ROWS), 0)
    col = lax.broadcasted_iota(jnp.int32, (ROWS, ROWS), 1)
    upto = jnp.where(col <= row, 1.0, 0.0).astype(jnp.bfloat16)
    upto = jnp.concatenate([upto, upto], axis=1)

    unit = math.log2(math.e) / length
    ends, sums_f, sums_b = [], [], []
    with jax.named_scope("local"):
        for pair in range(blocks // 2):
            if (pair * 2 * ROWS) % part == 0:
                for load in loads[pair * 2 * ROWS // part]:
                    load.wait()
            two = [pl.ds((2 * pair + side) * ROWS, ROWS) for side in (0, 1)]
            pieces = [split(leak[rows]) for rows in two]
            summed = jnp.dot(
                upto,
                jnp.concatenate(
                    [jnp.concatenate([p[k] for p in pieces], axis=1) for k in (0, 1)], axis=0
                ),
                preferred_element_type=f32,
            )
            for side in (0, 1):
                rows = two[side]
                inside = summed[:, side * ROWS : (side + 1) * ROWS]
                wide = signal[rows].astype(f32)
                up_f = jnp.exp2(inside * unit)
                up_b = jnp.exp2((leak[rows] - inside) * unit)
                through[rows], grow_f[rows], grow_b[rows] = inside, up_f, up_b
                ends.append(jnp.exp2(inside[ROWS - 1 :] * -unit))
                sums_f.append(ends[-1] * jnp.sum(wide * up_f, axis=0, keepdims=True))
                sums_b.append(jnp.sum(wide * up_b, axis=0, keepdims=True))

    with jax.named_scope("ends"):
        at, product = jnp.zeros_like(ends[0]), jnp.ones_like(ends[0])
        for b in range(blocks):
            carried_f[b : b + 1] = at
            decayed_f[b : b + 1] = product
            at, product = at * ends[b] + sums_f[b], product * ends[b]
        own_carry[0:1] = product
        own_carry[1:2] = at
        at, product = jnp.zeros_like(ends[0]), jnp.ones_like(ends[0])
        for b in reversed(range(blocks)):
            at, product = at * ends[b] + sums_b[b], product * ends[b]
            carried_b[b : b + 1] = at
            decayed_b[b : b + 1] = product
        own_carry[2:3] = at
        got_carry[seq] = own_carry[...]


    with jax.named_scope("barrier"):
        pl.semaphore_wait(barrier, seq_n + width_n - 2)


    sends = []
    with jax.named_scope("send_carry"):
        for k, other in enumerate(seq_partners):
            sends.append(pltpu.make_async_remote_copy(
                src_ref=own_carry, dst_ref=got_carry.at[seq],
                send_sem=carry_send.at[k], recv_sem=carry_recv.at[k],
                device_id={"seq": other}, device_id_type=MESH,
            ))
            sends[-1].start()

    with jax.named_scope("inner"):
        for b in range(blocks):
            rows = pl.ds(b * ROWS, ROWS)
            push = signal[rows]
            wide, inside = push.astype(f32), through[rows]
            extra_f = (wide * (grow_f[rows] - 1.0)).astype(jnp.bfloat16)
            extra_b = (wide * (grow_b[rows] - 1.0)).astype(jnp.bfloat16)
            both = jnp.dot(
                upto,
                jnp.concatenate(
                    [
                        jnp.concatenate([push, push], axis=1),
                        jnp.concatenate([extra_f, extra_b], axis=1),
                    ],
                    axis=0,
                ),
                preferred_element_type=f32,
            )
            down, up = jnp.exp2(inside * -unit), jnp.exp2((inside - leak[rows]) * unit)
            decay[rows], grow[rows] = down, up
            states[rows] = down * both[:, :ROWS] + (wide - up * both[:, ROWS:])

    with jax.named_scope("wait_carry"):
        for send in sends:
            send.wait_recv()

    with jax.named_scope("enter"):
        into_f, into_b = jnp.zeros_like(ends[0]), jnp.zeros_like(ends[0])
        for j in range(seq_n):
            into_f = jnp.where(j < seq, into_f * got_carry[j, 0:1] + got_carry[j, 1:2], into_f)
            i = seq_n - 1 - j
            into_b = jnp.where(i > seq, into_b * got_carry[i, 0:1] + got_carry[i, 2:3], into_b)
        carried_f[...] = carried_f[...] + decayed_f[...] * into_f
        carried_b[...] = carried_b[...] + decayed_b[...] * into_b


    with jax.named_scope("power"):
        ones = jnp.ones((8, 2 * ROWS), jnp.bfloat16)
        for pair in range(blocks // 2):
            squares = []
            for b in (2 * pair, 2 * pair + 1):
                rows = pl.ds(b * ROWS, ROWS)
                value = (
                    states[rows]
                    + decay[rows] * carried_f[b : b + 1]
                    + grow[rows] * carried_b[b : b + 1]
                )
                states[rows] = value
                squares.append(jnp.concatenate(split(value * value), axis=1))
            power = lax.dot_general(
                ones, jnp.concatenate(squares, axis=0), NT, preferred_element_type=f32
            )
            own_power[2 * pair : 2 * pair + 1] = power[0:1, :ROWS]
            own_power[2 * pair + 1 : 2 * pair + 2] = power[0:1, ROWS:]
        got_power[width] = own_power[...]


    with jax.named_scope("send_power"):
        for k, other in enumerate(width_partners):
            send = pltpu.make_async_remote_copy(
                src_ref=own_power, dst_ref=got_power.at[width],
                send_sem=power_send.at[k], recv_sem=power_recv.at[k],
                device_id={"width": other}, device_id_type=MESH,
            )
            send.start()
            sends.append(send)


    with jax.named_scope("gain"):
        gain_load.wait()
        by = gain[...] * length**-0.5
        for b in range(blocks):
            rows = pl.ds(b * ROWS, ROWS)
            states[rows] = states[rows] * by


    with jax.named_scope("wait_power"):
        for send in sends[seq_n - 1 :]:
            send.wait_recv()


    with jax.named_scope("total"):
        total = got_power[0]
        for j in range(1, width_n):
            total = total + got_power[j]
        scale_ref[...] = lax.rsqrt(total * (1.0 / (channels * length)) + 1e-06)

    with jax.named_scope("drain"):
        for send in sends:
            send.wait_send()


def finish(states, scale_ref, out_hbm, out, out_sem):
    blocks, lanes = scale_ref.shape
    parts = out_sem.shape[0]
    part = out.shape[0] // parts
    zeros = jnp.zeros((lanes - blocks, lanes), jnp.float32)
    scale = jnp.concatenate([scale_ref[...], zeros], axis=0).T
    stores = []
    for b in range(blocks):
        rows = pl.ds(b * ROWS, ROWS)
        out[rows] = (states[rows] * scale[:, b : b + 1]).astype(out.dtype)
        if (b + 1) * ROWS % part == 0:
            k = (b + 1) * ROWS // part - 1
            rows = pl.ds(k * part, part)
            stores.append(pltpu.make_async_copy(out.at[rows], out_hbm.at[rows], out_sem.at[k]))
            stores[-1].start()
    for store in stores:
        store.wait()


def solution(mesh):
    sizes = dict(mesh.shape)
    seq_n, width_n = sizes["seq"], sizes["width"]
    seq_sizes, width_sizes = (4, seq_n // 4), (width_n // 2, 2)

    def per_device(leak_rate, signal_in, norm_gain):
        _, rows, lanes = leak_rate.shape
        length, channels = rows * seq_n, lanes * width_n
        blocks = rows // ROWS
        f32 = jnp.float32
        vmem, dma = pltpu.VMEM, pltpu.SemaphoreType.DMA
        here = pl.BlockSpec(memory_space=pltpu.VMEM)
        there = pl.BlockSpec(memory_space=pl.ANY)
        states, scale = pl.pallas_call(
            functools.partial(kernel, length, channels, seq_sizes, width_sizes),
            out_shape=[pltpu.VMEM((rows, lanes), f32), pltpu.VMEM((blocks, lanes), f32)],
            in_specs=[there] * 3,
            out_specs=[here, here],
            scratch_shapes=[
                vmem((rows, lanes), f32),
                vmem((rows, lanes), jnp.bfloat16),
                vmem((1, lanes), f32),
                *[vmem((rows, lanes), f32)] * 5,
                *[vmem((blocks, lanes), f32)] * 4,
                vmem((3, lanes), f32),
                vmem((seq_n, 3, lanes), f32),
                vmem((blocks, lanes), f32),
                vmem((width_n, blocks, lanes), f32),
                dma((2, 4)),
                dma,
                dma((seq_n - 1,)),
                dma((seq_n - 1,)),
                dma((width_n - 1,)),
                dma((width_n - 1,)),
            ],
            compiler_params=pltpu.CompilerParams(collective_id=0, has_side_effects=True),
            name="scan_norm",
        )(leak_rate[0], signal_in[0], norm_gain[None])
        out = pl.pallas_call(
            finish,
            out_shape=jax.ShapeDtypeStruct((rows, lanes), jnp.bfloat16),
            in_specs=[here, here],
            out_specs=there,
            scratch_shapes=[vmem((rows, lanes), jnp.bfloat16), dma((4,))],
            compiler_params=pltpu.CompilerParams(vmem_limit_bytes=8 << 20),
            name="finish",
        )(states, scale)
        return out[None]

    return jax.shard_map(
        per_device,
        mesh=mesh,
        in_specs=(P(None, "seq", "width"), P(None, "seq", "width"), P("width")),
        out_specs=P(None, "seq", "width"),
        check_vma=False,
    )
```
